32 devices in a mesh: gx: 4 (over y, x), gy: 4 (over z), gz: 2 (over core).
Axes of the slice: x: 2, y: 2, z: 4, core: 2. Of those that a mesh axis runs over, the one named last changes fastest.
Arguments:
- seg_rows: bfloat16 [4096, 128, 128], P(('gx', 'gy', 'gz')), may hold values from -6 to 6
- owner_map: int32 [4096, 1], replicated, may hold values from 0 to 31; in each aligned block of 128 rows (0 to 127, 128 to 255, ...) at most 8 rows name the same one
- ghost_pick: int32 [32, 1], P(('gx', 'gy', 'gz')), may hold values from 0 to 127
- slab_cost: int32 [4, 4, 2, 3, 1024], P('gx', 'gy', 'gz'), may hold values from 1 to 24
Outputs:
- forces: bfloat16 [32, 32, 8, 128, 128], P(('gx', 'gy', 'gz'))
- cut_points: float32 [7], replicated
The draws below stay inside these ranges and needn't reach their ends.
Inputs may be any that keep to these rules, and one draw needn't show every extreme that they name: `owner_map`: among the 128 blocks of one device (aligned runs of 128 rows) no owner is named more than 8 times; some device names some owner exactly 8 times.
All inputs are finite; a program needn't handle non-finite values.
Results may differ from the reference program's by a relative error of at most 0.0034.
Values may be sent and summed in bfloat16 or wider, within the bound.
A program may use at most 128 MiB of HBM per device.

```python
import math
import jax
import jax.numpy as jnp
import numpy as np
from jax import lax

W = 128
BLK = 128
BLK_DEV = 128
GH = 1
NSLAB = 1024
BLOCKS = 4096
CAP = 8
N_GX = 4
N_GY = 4
N_GZ = 2
DEVICES = 32


def draw_slab_cost(key, part):
    full_shape = (N_GX, N_GY, N_GZ, 3, NSLAB)
    coord_x = lax.broadcasted_iota(jnp.int32, full_shape, 0)
    coord_y = lax.broadcasted_iota(jnp.int32, full_shape, 1)
    coord_z = lax.broadcasted_iota(jnp.int32, full_shape, 2)
    direction = lax.broadcasted_iota(jnp.int32, full_shape, 3)
    slab_index = lax.broadcasted_iota(jnp.int32, full_shape, 4)
    flat_dev = (coord_x * N_GY + coord_y) * N_GZ + coord_z
    own_coord = jnp.where(direction == 0, coord_x, jnp.where(direction == 1, coord_y, coord_z))
    extent = jnp.where(direction == 0, N_GX, jnp.where(direction == 1, N_GY, N_GZ))
    region = slab_index * extent // NSLAB
    hot_key = jax.random.fold_in(key, 11)
    cost_key = jax.random.fold_in(key, 23)
    hotness = jax.random.randint(hot_key, (N_GX, N_GY, N_GZ, 3, 1), 1, 9, dtype=jnp.int32)
    ceiling = jnp.where(region == own_coord, 1 + hotness * (DEVICES + 2 * flat_dev) // DEVICES, 1)
    return jax.random.randint(cost_key, full_shape, 1, ceiling + 1, dtype=jnp.int32)


def place_ends(values, own_key, smallest, high):
    index_at = [jax.random.randint(jax.random.fold_in(own_key, axis), (), 0, length) for axis, length in enumerate(values.shape)]
    widest = values.shape.index(max(values.shape))
    beside = index_at[:widest] + [(index_at[widest] + 1) % values.shape[widest]] + index_at[widest + 1:]
    return values.at[tuple(index_at)].set(smallest).at[tuple(beside)].set(high)


def levels(own_key, shape, pieces, least, largest):
    loudness, own = 1.0, jax.random.fold_in(own_key, 6)
    for dim, parts in pieces:
        draws = jnp.exp(jax.random.uniform(jax.random.fold_in(own, dim), (parts,), jnp.float32, least / len(pieces), largest / len(pieces)))
        loudness = loudness * jnp.repeat(draws, shape[dim] // parts).reshape([-1 if axis == dim else 1 for axis in range(len(shape))])
    return loudness


def deal_out(key, own, number, rows, count, top, most, skew):
    ranking = jax.random.permutation(key, count)
    crowded, common = portions_of(count, rows * top, most, skew, True), portions_of(count, rows * top, most, skew, False)
    places = jnp.arange(count)

    def named(sizes, offset_by):
        used = int((sizes > 0).sum())
        fixed = max(1, used // 4)
        passed = fixed + (places - fixed + offset_by * (used - fixed)) % max(1, count - fixed)
        return jnp.zeros((count,), jnp.int32).at[ranking[jnp.where(places < fixed, places, passed)]].set(jnp.asarray(sizes, jnp.int32))

    sizes = jnp.where(number % 4 == 0, named(crowded, number // 4), named(common, number - number // 4 - 1))
    mixed = jax.random.permutation(jax.random.fold_in(own, 3), count)
    source_of, receiver = mixed[0:count // 2 * 2:2], mixed[1:count // 2 * 2:2]
    slack = jnp.minimum(sizes[source_of] - 1, most - sizes[receiver]) // 2
    slack = jnp.where((source_of == ranking[0]) | (receiver == ranking[0]) | (sizes[receiver] == 0), 0, jnp.maximum(slack, 0))
    passed = jax.random.randint(jax.random.fold_in(own, 4), (count // 2,), 0, 1 << 20) % (slack + 1)
    sizes = sizes.at[source_of].add(-passed).at[receiver].add(passed)
    labels = jnp.searchsorted(jnp.cumsum(sizes), jnp.arange(rows * top), side="right").astype(jnp.int32)
    listing = labels.reshape(top, rows).T
    listing = listing[jax.random.permutation(jax.random.fold_in(own, 1), rows)]
    offset_by = jax.random.randint(jax.random.fold_in(own, 2), (rows, 1), 0, top)
    return jnp.take_along_axis(listing, (jnp.arange(top)[None, :] + offset_by) % top, axis=1)


def portions_of(count, total, limit, lean, full):
    loads = [(1 << 20) // math.isqrt(rank ** lean) + 1 for rank in range(1, count + 1)]
    largest = limit if full else min(limit, max(-(-total // count), total * loads[0] // sum(loads)))
    least = 1 if total - largest >= count - 1 else 0
    holding, spare = [largest] + [least] * (count - 1), total - largest - least * (count - 1)
    while spare > 0:
        movable = [i for i in range(1, count) if holding[i] < largest] or [i for i in range(1, count) if holding[i] < limit]
        whole, left = sum([loads[i] for i in movable]), spare
        for i in movable:
            more = min(limit - holding[i], max(1, left * loads[i] // whole), spare)
            holding[i] = holding[i] + more
            spare = spare - more
    return np.array(holding)


def noise(key, shape, scale, limit, split=(), kind=jnp.bfloat16):
    factor_of = levels(key, shape, split, -0.22, 0.18) if split else 1.0
    values = jax.random.normal(key, shape, jnp.float32) * scale * factor_of
    return jnp.minimum(jnp.maximum(values, -limit), limit).astype(kind)


def setup_inputs(seed: int = 0) -> dict:
    keys = jax.random.split(jax.random.key(seed), 5)
    seg_rows = noise(keys[0], (BLOCKS, BLK, W), 1.0, 6.0, ((0, 32),))
    owner_map_keys = jax.random.split(jax.random.fold_in(keys[1], 1), BLOCKS // BLK_DEV)
    owner_map_turns = jax.random.permutation(jax.random.fold_in(keys[1], 3), BLOCKS // BLK_DEV)
    owner_map = jax.vmap(lambda own, number: deal_out(jax.random.fold_in(keys[1], 2), own, number, BLK_DEV, DEVICES, 1, CAP, 2))(owner_map_keys, owner_map_turns).reshape((BLOCKS, 1))
    ghost_pick = place_ends(jax.random.randint(keys[2], (DEVICES, GH), 0, BLK_DEV), jax.random.fold_in(keys[2], 1), 0, BLK_DEV - 1).astype(jnp.int32)
    slab_cost = draw_slab_cost(jax.random.fold_in(keys[4], 71), 0)
    return dict(seg_rows=seg_rows, owner_map=owner_map, ghost_pick=ghost_pick, slab_cost=slab_cost)


sharpness = 8.0
force_gain = 2.0
radius_eps = 1e-3


def bisect_cuts(histogram):
    running = jnp.cumsum(histogram, axis=1, dtype=jnp.int32)
    total_cost = running[:, -1]
    below = (2 * running < total_cost[:, None]).astype(jnp.int32)
    position = jnp.sum(below, axis=1, dtype=jnp.int32)
    before = jnp.sum(histogram * below, axis=1, dtype=jnp.int32)
    bins_index = lax.broadcasted_iota(jnp.int32, histogram.shape, 1)
    at_cut = jnp.sum(jnp.where(bins_index == position[:, None], histogram, 0), axis=1, dtype=jnp.int32)
    remain = (total_cost - 2 * before).astype(jnp.float32)
    return (position.astype(jnp.float32) + remain / (2 * at_cut).astype(jnp.float32)) / histogram.shape[1]


def kernel_weights(left_sq, right_sq, inner):
    spread = left_sq + right_sq - 2.0 * inner
    return jnp.exp(-sharpness * spread / (left_sq + right_sq + radius_eps)).astype(jnp.bfloat16)


def block_forces(block_rows, ghost_rows):
    rows_f = block_rows.astype(jnp.float32)
    ghosts_f = ghost_rows.astype(jnp.float32)
    own_sq = jnp.sum(rows_f * rows_f, axis=-1)
    ghost_sq = jnp.sum(ghosts_f * ghosts_f, axis=-1)
    own_inner = jnp.einsum("sbw,scw->sbc", rows_f, rows_f, precision=lax.Precision.HIGHEST)
    ghost_inner = jnp.einsum("sbw,smw->sbm", rows_f, ghosts_f, precision=lax.Precision.HIGHEST)
    own_kernel = kernel_weights(own_sq[:, :, None], own_sq[:, None, :], own_inner)
    ghost_kernel = kernel_weights(own_sq[:, :, None], ghost_sq[:, None, :], ghost_inner)
    own_kf = own_kernel.astype(jnp.float32)
    ghost_kf = ghost_kernel.astype(jnp.float32)
    weight_sum = jnp.sum(own_kf, axis=-1) + jnp.sum(ghost_kf, axis=-1)
    pulled = jnp.einsum("sbc,scw->sbw", own_kf, rows_f, precision=lax.Precision.HIGHEST)
    pulled = pulled + jnp.einsum("sbm,smw->sbw", ghost_kf, ghosts_f, precision=lax.Precision.HIGHEST)
    return (force_gain * (pulled - weight_sum[..., None] * rows_f)).astype(jnp.bfloat16)


def flat_index(coord_x, coord_y, coord_z):
    return ((coord_x % N_GX) * N_GY + coord_y % N_GY) * N_GZ + coord_z % N_GZ


def reference(seg_rows, owner_map, ghost_pick, slab_cost):
    hist_x = jnp.sum(slab_cost[:, :, :, 0, :], axis=(0, 1, 2), dtype=jnp.int32)[None]
    hist_y = jnp.sum(slab_cost[:, :, :, 1, :].reshape(2, N_GX // 2, N_GY, N_GZ, NSLAB), axis=(1, 2, 3), dtype=jnp.int32)
    hist_z = jnp.sum(slab_cost[:, :, :, 2, :].reshape(2, N_GX // 2, 2, N_GY // 2, N_GZ, NSLAB), axis=(1, 3, 4), dtype=jnp.int32).reshape(4, NSLAB)
    histogram = jnp.concatenate([hist_x, hist_y, hist_z], axis=0)
    extent = jnp.array([N_GX, N_GY, N_GY, N_GZ, N_GZ, N_GZ, N_GZ], jnp.float32)
    cut_points = bisect_cuts(histogram) * extent

    owners = owner_map[:, 0].reshape(DEVICES, BLK_DEV)
    block_order = jnp.arange(BLK_DEV, dtype=jnp.int32)
    earlier = block_order[:, None] < block_order[None, :]
    same_owner = owners[:, :, None] == owners[:, None, :]
    slot_rank = jnp.sum((same_owner & earlier[None]).astype(jnp.int32), axis=1, dtype=jnp.int32)

    grouped_rows = seg_rows.reshape(DEVICES, BLK_DEV, BLK, W)
    exported = jnp.take_along_axis(grouped_rows, ghost_pick[:, :, None, None], axis=1)
    device = jnp.arange(DEVICES, dtype=jnp.int32)
    along_x = device // (N_GY * N_GZ)
    along_y = (device // N_GZ) % N_GY
    along_z = device % N_GZ
    neighbour = jnp.stack([
        flat_index(along_x - 1, along_y, along_z), flat_index(along_x + 1, along_y, along_z),
        flat_index(along_x, along_y - 1, along_z), flat_index(along_x, along_y + 1, along_z),
        flat_index(along_x, along_y, along_z - 1), flat_index(along_x, along_y, along_z + 1)], axis=1)
    ghost_all = exported[neighbour].reshape(DEVICES, 6 * GH * BLK, W)

    owner_flat = owner_map[:, 0]
    group_size = math.gcd(BLOCKS, 16)

    def per_group(operands):
        rows_group, dest_group = operands
        return block_forces(rows_group, ghost_all[dest_group])

    forces_blocks = lax.map(per_group, (seg_rows.reshape(BLOCKS // group_size, group_size, BLK, W), owner_flat.reshape(BLOCKS // group_size, group_size)))
    forces_blocks = forces_blocks.reshape(BLOCKS, BLK, W)
    source = jnp.arange(BLOCKS, dtype=jnp.int32) // BLK_DEV
    forces = jnp.zeros((DEVICES, DEVICES, CAP, BLK, W), jnp.bfloat16)
    forces = forces.at[owner_flat, source, slot_rank.reshape(-1)].set(forces_blocks)
    return forces, cut_points
```

```python
import functools
import math

import jax
import jax.numpy as jnp
from jax import lax
from jax.experimental import pallas as pl
from jax.experimental.pallas import tpu as pltpu
from jax.sharding import PartitionSpec as P

sharpness = 8.0
force_gain = 2.0
radius_eps = 0.001
AXES = ("gx", "gy", "gz")
MESH = pl.DeviceIdType.MESH
LANES = 128


def bisect_cuts(histogram):
    running = jnp.cumsum(histogram, axis=1, dtype=jnp.int32)
    total_cost = running[:, -1]
    below = (2 * running < total_cost[:, None]).astype(jnp.int32)
    position = jnp.sum(below, axis=1, dtype=jnp.int32)
    before = jnp.sum(histogram * below, axis=1, dtype=jnp.int32)
    bins_index = lax.broadcasted_iota(jnp.int32, histogram.shape, 1)
    at_cut = jnp.sum(
        jnp.where(bins_index == position[:, None], histogram, 0), axis=1, dtype=jnp.int32
    )
    remain = (total_cost - 2 * before).astype(jnp.float32)
    return (
        position.astype(jnp.float32) + remain / (2 * at_cut).astype(jnp.float32)
    ) / histogram.shape[1]


def pack_kernel(capacity, source_ref, rows_ref, out_ref):
    owner = pl.program_id(0)
    for slot in range(capacity):
        out_ref[0, slot] = rows_ref[source_ref[owner * capacity + slot]]


def pack_slots(seg_rows, source_block, device_count, capacity):
    _, block_rows, width = seg_rows.shape
    return pl.pallas_call(
        functools.partial(pack_kernel, capacity),
        out_shape=jax.ShapeDtypeStruct((device_count, capacity, block_rows, width), seg_rows.dtype),
        grid_spec=pltpu.PrefetchScalarGridSpec(
            num_scalar_prefetch=1,
            grid=(device_count,),
            in_specs=[pl.BlockSpec(memory_space=pltpu.VMEM)],
            out_specs=pl.BlockSpec(
                (1, capacity, block_rows, width), lambda owner, source: (owner, 0, 0, 0)
            ),
        ),
        name="pack_slots",
    )(source_block, seg_rows)


def square_parts(inner):
    rows = lax.broadcasted_iota(jnp.int32, inner.shape, 0)
    columns = lax.broadcasted_iota(jnp.int32, inner.shape, 1)
    diagonal = jnp.where(rows == columns, inner, 0.0)
    return jnp.sum(diagonal, axis=1, keepdims=True), jnp.sum(diagonal, axis=0, keepdims=True)


def dot_t(left, right):
    return lax.dot_general(
        left, right, (((1,), (1,)), ((), ())), preferred_element_type=jnp.float32
    )


def pair_weights(left_sq, right_sq, inner):
    scale = sharpness * math.log2(math.e)
    ratio = (2.0 * inner + radius_eps) / (left_sq + (right_sq + radius_eps))
    return jnp.exp2(scale * ratio - scale).astype(jnp.bfloat16)


def relay_kernel(
    sizes, capacity, group,
    gain_ref, outgoing_ref, export_ref, cost_ref,
    forces_ref, hist_ref,
    held, ghosts, ghost_aug, ghost_sq, own_aug, hist_cur, hist_in,
    send_sem, recv_sem, out_sem, own_sem, gsend_sem, grecv_sem, hsend_sem, hrecv_sem,
):
    count_x, count_y, count_z = sizes
    device_count = count_x * count_y * count_z
    block_rows, width = export_ref.shape
    coords = tuple(lax.axis_index(axis) for axis in AXES)
    me = (coords[0] * count_y + coords[1]) * count_z + coords[2]

    def coords_of(flat):
        return (flat // (count_y * count_z), (flat // count_z) % count_y, flat % count_z)

    def shifted(axis, offset):
        place = list(coords)
        place[axis] = (coords[axis] + offset + sizes[axis]) % sizes[axis]
        return tuple(place)

    barrier = pltpu.get_barrier_semaphore()

    @pl.loop(1, device_count)
    def _(k):
        pl.semaphore_signal(
            barrier, inc=1, device_id=coords_of((me + k) % device_count), device_id_type=MESH
        )

    pl.semaphore_wait(barrier, device_count - 1)

    ghost_copies = []
    for axis in range(3):
        for side, offset in ((0, 1), (1, -1)):
            index = 2 * axis + side
            copy = pltpu.make_async_remote_copy(
                src_ref=export_ref,
                dst_ref=ghosts.at[pl.ds(index * block_rows, block_rows)],
                send_sem=gsend_sem.at[index],
                recv_sem=grecv_sem.at[index],
                device_id=shifted(axis, offset),
                device_id_type=MESH,
            )
            copy.start()
            ghost_copies.append(copy)

    stage_axes = (1, 0, 2)
    bases = []
    total = 0
    for axis in stage_axes:
        bases.append(total)
        total += sizes[axis] - 1

    def hist_copies(stage):
        axis = stage_axes[stage]
        return [
            pltpu.make_async_remote_copy(
                src_ref=cost_ref if stage == 0 else hist_cur.at[stage - 1],
                dst_ref=hist_in.at[bases[stage] + offset - 1],
                send_sem=hsend_sem.at[bases[stage] + offset - 1],
                recv_sem=hrecv_sem.at[bases[stage] + offset - 1],
                device_id=shifted(axis, offset),
                device_id_type=MESH,
            )
            for offset in range(1, sizes[axis])
        ]

    def hist_start(stage):
        for copy in hist_copies(stage):
            copy.start()

    def hist_finish(stage):
        summed = cost_ref[...] if stage == 0 else hist_cur[stage - 1]
        for index, copy in enumerate(hist_copies(stage)):
            copy.wait()
            summed = summed + hist_in[bases[stage] + index]
        if stage == 2:
            hist_ref[...] = summed
        else:
            hist_cur[stage] = summed

    hist_start(0)

    def big_copy(k):
        target = (me + k) % device_count
        return pltpu.make_async_remote_copy(
            src_ref=outgoing_ref.at[target],
            dst_ref=held.at[me],
            send_sem=send_sem.at[k],
            recv_sem=recv_sem.at[k],
            device_id=coords_of(target),
            device_id_type=MESH,
        )

    def arrival(k):
        source = (me - k + device_count) % device_count
        return pltpu.make_async_remote_copy(
            src_ref=outgoing_ref.at[source],
            dst_ref=held.at[source],
            send_sem=send_sem.at[k],
            recv_sem=recv_sem.at[k],
            device_id=coords_of(source),
            device_id_type=MESH,
        )

    @pl.loop(1, device_count)
    def _(k):
        big_copy(k).start()

    own_copy = pltpu.make_async_copy(outgoing_ref.at[me], held.at[me], own_sem)
    own_copy.start()

    ghost_aug[:, width:] = jnp.ones((ghost_aug.shape[0], width), jnp.bfloat16)
    own_aug[:, :, width:] = jnp.ones((group, block_rows, width), jnp.bfloat16)
    for copy in ghost_copies:
        copy.wait()
    for index in range(6):
        piece = ghosts[pl.ds(index * block_rows, block_rows), :]
        ghost_aug[pl.ds(index * block_rows, block_rows), pl.ds(0, width)] = piece
        _, row_sq = square_parts(dot_t(piece, piece))
        ghost_sq[:, pl.ds(index * block_rows, block_rows)] = row_sq

    own_copy.wait()

    def out_copy(source):
        return pltpu.make_async_copy(held.at[source], forces_ref.at[source], out_sem.at[source])

    @pl.loop(0, device_count)
    def _(k):
        source = (me - k + device_count) % device_count

        @pl.when(k > 0)
        def _():
            arrival(k).wait_recv()

        @pl.loop(0, capacity // group)
        def _(part):
            for inside in range(group):
                slot = part * group + inside
                rows = held[source, slot]
                own_aug[inside, :, pl.ds(0, width)] = rows
                own_inner = dot_t(rows, rows)
                left_sq, right_sq = square_parts(own_inner)
                own_weight = pair_weights(left_sq, right_sq, own_inner)
                ghost_weight = pair_weights(left_sq, ghost_sq[...], dot_t(rows, ghosts[...]))
                pulled = jnp.dot(
                    own_weight, own_aug[inside], preferred_element_type=jnp.float32
                ) + jnp.dot(ghost_weight, ghost_aug[...], preferred_element_type=jnp.float32)
                gain = gain_ref[source * capacity + slot]
                forces = gain * (
                    pulled[:, :width] - pulled[:, width:] * rows.astype(jnp.float32)
                )
                held[source, slot] = forces.astype(jnp.bfloat16)

        out_copy(source).start()
        for stage in range(3):

            @pl.when(k == (stage * device_count) // 4)
            def _():
                hist_finish(stage)
                if stage < 2:
                    hist_start(stage + 1)

    @pl.loop(1, device_count)
    def _(k):
        big_copy(k).wait_send()

    @pl.loop(0, device_count)
    def _(source):
        out_copy(source).wait()


def per_device(seg_rows, owner_map, ghost_pick, slab_cost):
    sizes = tuple(lax.axis_size(axis) for axis in AXES)
    count_x, count_y, count_z = sizes
    device_count = count_x * count_y * count_z
    blocks_here, block_rows, width = seg_rows.shape
    capacity = max(2, (2 * blocks_here + device_count - 1) // device_count)
    own_index = lax.axis_index(AXES)
    index_x = lax.axis_index("gx")
    index_y = lax.axis_index("gy")
    local_cost = slab_cost[0, 0, 0]
    bins_count = local_cost.shape[1]
    half_part = index_x // (count_x // 2)
    quarter = half_part * 2 + index_y // (count_y // 2)
    x_term = local_cost[0][None]
    y_term = jnp.where(
        lax.broadcasted_iota(jnp.int32, (2, bins_count), 0) == half_part, local_cost[1][None], 0
    )
    z_term = jnp.where(
        lax.broadcasted_iota(jnp.int32, (4, bins_count), 0) == quarter, local_cost[2][None], 0
    )
    terms = jnp.concatenate([x_term, y_term, z_term], axis=0).reshape(-1, LANES)
    exported = jnp.take(seg_rows, ghost_pick[0], axis=0)[0]

    all_owners = owner_map[:, 0].reshape(device_count, blocks_here)
    own_owners = lax.dynamic_index_in_dim(all_owners, own_index, 0, keepdims=False)
    block_order = lax.broadcasted_iota(jnp.int32, (blocks_here,), 0)
    earlier = block_order[:, None] < block_order[None, :]
    same_owner = own_owners[:, None] == own_owners[None, :]
    slot_rank = jnp.sum((same_owner & earlier).astype(jnp.int32), axis=0, dtype=jnp.int32)
    slot_of = own_owners * capacity + slot_rank
    slot_ids = lax.broadcasted_iota(jnp.int32, (device_count * capacity,), 0)
    matches = slot_of[None, :] == slot_ids[:, None]
    source_block = jnp.sum(jnp.where(matches, block_order[None, :], 0), axis=1, dtype=jnp.int32)
    arrivals = jnp.sum((all_owners == own_index).astype(jnp.int32), axis=1, dtype=jnp.int32)
    valid_slot = lax.broadcasted_iota(jnp.int32, (device_count, capacity), 1) < arrivals[:, None]
    gain = jnp.where(valid_slot, force_gain, 0.0).astype(jnp.float32).reshape(-1)

    outgoing = pack_slots(seg_rows, source_block, device_count, capacity)

    group = math.gcd(capacity, 2)
    ghost_rows = 6 * block_rows
    hist_rows = terms.shape[0]
    hist_messages = sum(sizes) - 3
    forces, hist = pl.pallas_call(
        functools.partial(relay_kernel, sizes, capacity, group),
        out_shape=(
            jax.ShapeDtypeStruct((device_count, capacity, block_rows, width), jnp.bfloat16),
            jax.ShapeDtypeStruct((hist_rows, LANES), jnp.int32),
        ),
        in_specs=[
            pl.BlockSpec(memory_space=pltpu.SMEM),
            pl.BlockSpec(memory_space=pl.ANY),
            pl.BlockSpec(memory_space=pltpu.VMEM),
            pl.BlockSpec(memory_space=pltpu.VMEM),
        ],
        out_specs=(
            pl.BlockSpec(memory_space=pl.ANY),
            pl.BlockSpec(memory_space=pltpu.VMEM),
        ),
        scratch_shapes=[
            pltpu.VMEM((device_count, capacity, block_rows, width), jnp.bfloat16),
            pltpu.VMEM((ghost_rows, width), jnp.bfloat16),
            pltpu.VMEM((ghost_rows, 2 * width), jnp.bfloat16),
            pltpu.VMEM((1, ghost_rows), jnp.float32),
            pltpu.VMEM((group, block_rows, 2 * width), jnp.bfloat16),
            pltpu.VMEM((2, hist_rows, LANES), jnp.int32),
            pltpu.VMEM((hist_messages, hist_rows, LANES), jnp.int32),
            pltpu.SemaphoreType.DMA((device_count,)),
            pltpu.SemaphoreType.DMA((device_count,)),
            pltpu.SemaphoreType.DMA((device_count,)),
            pltpu.SemaphoreType.DMA,
            pltpu.SemaphoreType.DMA((6,)),
            pltpu.SemaphoreType.DMA((6,)),
            pltpu.SemaphoreType.DMA((hist_messages,)),
            pltpu.SemaphoreType.DMA((hist_messages,)),
        ],
        compiler_params=pltpu.CompilerParams(collective_id=0, has_side_effects=True),
        name="relay_forces",
    )(gain, outgoing, exported, terms)
    extent = jnp.array([count_x, count_y, count_y, count_z, count_z, count_z, count_z], jnp.float32)
    cut_points = bisect_cuts(hist.reshape(-1, bins_count)) * extent
    return (forces[None], cut_points)


def solution(mesh):
    return jax.shard_map(
        per_device,
        mesh=mesh,
        in_specs=(
            P(AXES, None, None),
            P(),
            P(AXES, None),
            P("gx", "gy", "gz", None, None),
        ),
        out_specs=(P(AXES, None, None, None, None), P()),
        check_vma=False,
    )
```

```python
import functools
import math

import jax
import jax.numpy as jnp
from jax import lax
from jax.experimental import pallas as pl
from jax.experimental.pallas import tpu as pltpu
from jax.sharding import PartitionSpec as P

sharpness = 8.0
force_gain = 2.0
radius_eps = 0.001
AXES = ("gx", "gy", "gz")
MESH = pl.DeviceIdType.MESH
LANES = 128
SHARES = (2, 3, 4, 8)


def bisect_cuts(histogram):
    running = jnp.cumsum(histogram, axis=1, dtype=jnp.int32)
    total_cost = running[:, -1]
    below = (2 * running < total_cost[:, None]).astype(jnp.int32)
    position = jnp.sum(below, axis=1, dtype=jnp.int32)
    before = jnp.sum(histogram * below, axis=1, dtype=jnp.int32)
    bins_index = lax.broadcasted_iota(jnp.int32, histogram.shape, 1)
    at_cut = jnp.sum(
        jnp.where(bins_index == position[:, None], histogram, 0), axis=1, dtype=jnp.int32
    )
    remain = (total_cost - 2 * before).astype(jnp.float32)
    return (
        position.astype(jnp.float32) + remain / (2 * at_cut).astype(jnp.float32)
    ) / histogram.shape[1]


def square_parts(inner):
    rows = lax.broadcasted_iota(jnp.int32, inner.shape, 0)
    columns = lax.broadcasted_iota(jnp.int32, inner.shape, 1)
    diagonal = jnp.where(rows == columns, inner, 0.0)
    return jnp.sum(diagonal, axis=1, keepdims=True), jnp.sum(diagonal, axis=0, keepdims=True)


def dot_t(left, right):
    return lax.dot_general(
        left, right, (((1,), (1,)), ((), ())), preferred_element_type=jnp.float32
    )


def pair_weights(left_sq, right_sq, inner):
    scale = sharpness * math.log2(math.e)
    ratio = (2.0 * inner + radius_eps) / (left_sq + (right_sq + radius_eps))
    return jnp.exp2(scale * ratio - scale).astype(jnp.bfloat16)


def relay_kernel(
    sizes, capacity, halves, group, limit,
    pack_ref, forward_ref, gain_ref, rows_ref, export_ref, cost_ref,
    forces_ref, hist_ref,
    held, stage_out, ghosts, ghost_aug, ghost_sq, own_aug, hist_cur, hist_in,
    send_sem, recv_sem, out_sem, zsend_sem, zrecv_sem,
    gsend_sem, grecv_sem, hsend_sem, hrecv_sem, *z_refs,
):
    count_x, count_y, count_z = sizes
    device_count = count_x * count_y * count_z
    plane = count_x * count_z
    part = capacity // halves
    plane_slots = plane * capacity
    first = plane * part
    block_rows, width = export_ref.shape
    coords = tuple(lax.axis_index(axis) for axis in AXES)
    me = (coords[0] * count_y + coords[1]) * count_z + coords[2]
    my_spot = coords[0] * count_z + coords[2]
    steps = halves * count_y
    bounds = [(0, first), (first, limit)][:halves]
    pieces = [(half, offset) for half in range(halves) for offset in range(1, count_y)]
    z_out = dict(zip(pieces, z_refs[: len(pieces)]))
    z_in = dict(zip(pieces, z_refs[len(pieces) :]))

    def coords_of(flat):
        return (flat // (count_y * count_z), (flat // count_z) % count_y, flat % count_z)

    def shifted(axis, offset):
        place = list(coords)
        place[axis] = (coords[axis] + offset + sizes[axis]) % sizes[axis]
        return tuple(place)

    barrier = pltpu.get_barrier_semaphore()

    @pl.loop(1, device_count)
    def _(k):
        pl.semaphore_signal(
            barrier, inc=1, device_id=coords_of((me + k) % device_count), device_id_type=MESH
        )

    def z_pack(half, offset):
        low, high = bounds[half]

        @pl.loop(0, high - low)
        def _(place):
            z_out[half, offset][place] = rows_ref[pack_ref[offset * plane_slots + low + place]]

    def z_copy(half, offset):
        index = pieces.index((half, offset))
        return pltpu.make_async_remote_copy(
            src_ref=z_out[half, offset],
            dst_ref=z_in[half, offset],
            send_sem=zsend_sem.at[index],
            recv_sem=zrecv_sem.at[index],
            device_id=shifted(1, offset),
            device_id_type=MESH,
        )

    z_pack(*pieces[0])
    pl.semaphore_wait(barrier, device_count - 1)

    ghost_copies = []
    for axis in range(3):
        for side, offset in ((0, 1), (1, -1)):
            index = 2 * axis + side
            copy = pltpu.make_async_remote_copy(
                src_ref=export_ref,
                dst_ref=ghosts.at[pl.ds(index * block_rows, block_rows)],
                send_sem=gsend_sem.at[index],
                recv_sem=grecv_sem.at[index],
                device_id=shifted(axis, offset),
                device_id_type=MESH,
            )
            copy.start()
            ghost_copies.append(copy)

    stage_axes = (1, 0, 2)
    bases = []
    total = 0
    for axis in stage_axes:
        bases.append(total)
        total += sizes[axis] - 1

    def hist_copies(stage):
        axis = stage_axes[stage]
        return [
            pltpu.make_async_remote_copy(
                src_ref=cost_ref if stage == 0 else hist_cur.at[stage - 1],
                dst_ref=hist_in.at[bases[stage] + offset - 1],
                send_sem=hsend_sem.at[bases[stage] + offset - 1],
                recv_sem=hrecv_sem.at[bases[stage] + offset - 1],
                device_id=shifted(axis, offset),
                device_id_type=MESH,
            )
            for offset in range(1, sizes[axis])
        ]

    def hist_start(stage):
        for copy in hist_copies(stage):
            copy.start()

    def hist_finish(stage):
        summed = cost_ref[...] if stage == 0 else hist_cur[stage - 1]
        for index, copy in enumerate(hist_copies(stage)):
            copy.wait()
            summed = summed + hist_in[bases[stage] + index]
        if stage == 2:
            hist_ref[...] = summed
        else:
            hist_cur[stage] = summed

    hist_start(0)
    for index, piece in enumerate(pieces):
        if index + 1 < len(pieces):
            z_pack(*pieces[index + 1])
        z_copy(*piece).start()

    def spot_shift(away):
        return (my_spot + away + plane) % plane

    def device_at(spot):
        return (spot // count_z, coords[1], spot % count_z)

    def source_at(spot, offset):
        row = (coords[1] - offset + count_y) % count_y
        return ((spot // count_z) * count_y + row) * count_z + spot % count_z

    def step_parts(step):
        return step // count_y, step % count_y

    def forward_copy(step, away):
        half, offset = step_parts(step)
        spot = spot_shift(away)
        return pltpu.make_async_remote_copy(
            src_ref=stage_out.at[step, away],
            dst_ref=held.at[source_at(my_spot, offset), pl.ds(half * part, part)],
            send_sem=send_sem.at[step * plane + away],
            recv_sem=recv_sem.at[step * plane + away],
            device_id=device_at(spot),
            device_id_type=MESH,
        )

    def arrival(step, away):
        half, offset = step_parts(step)
        spot = spot_shift(-away)
        return pltpu.make_async_remote_copy(
            src_ref=stage_out.at[step, away],
            dst_ref=held.at[source_at(spot, offset), pl.ds(half * part, part)],
            send_sem=send_sem.at[step * plane + away],
            recv_sem=recv_sem.at[step * plane + away],
            device_id=device_at(spot),
            device_id_type=MESH,
        )

    def slot_value(half, offset, spot, inside):
        index = spot * capacity + half * part + inside
        if offset == 0:
            return rows_ref[pack_ref[index]]
        place = forward_ref[offset * plane_slots + index]
        if half == 0:
            return z_in[0, offset][place]
        early = z_in[0, offset][jnp.minimum(place, first - 1)]
        late = z_in[1, offset][jnp.clip(place - first, 0, limit - first - 1)]
        is_early = jnp.full(early.shape, place, jnp.int32) < first
        return jnp.where(is_early, early, late)

    def forward(half, offset):
        step = half * count_y + offset
        if offset > 0:
            z_copy(half, offset).wait_recv()

        @pl.loop(1, plane)
        def _(away):
            for inside in range(part):
                stage_out[step, away, inside] = slot_value(half, offset, spot_shift(away), inside)

            @pl.when(away > 1)
            def _():
                forward_copy(step, away - 1).start()

        own = source_at(my_spot, offset)
        for inside in range(part):
            held[own, half * part + inside] = slot_value(half, offset, my_spot, inside)
        forward_copy(step, plane - 1).start()

    def out_copy(step, away):
        half, offset = step_parts(step)
        source = source_at(spot_shift(-away), offset)
        return pltpu.make_async_copy(
            held.at[source, pl.ds(half * part, part)],
            forces_ref.at[source, pl.ds(half * part, part)],
            out_sem.at[step * plane + away],
        )

    def compute(step):
        half, offset = step_parts(step)

        @pl.loop(0, plane)
        def _(away):
            source = source_at(spot_shift(-away), offset)

            @pl.when(away > 0)
            def _():
                arrival(step, away).wait_recv()

            @pl.loop(0, part // group)
            def _(pair):
                for inside in range(group):
                    slot = half * part + pair * group + inside
                    rows = held[source, slot]
                    own_aug[inside, :, pl.ds(0, width)] = rows
                    own_inner = dot_t(rows, rows)
                    left_sq, right_sq = square_parts(own_inner)
                    own_weight = pair_weights(left_sq, right_sq, own_inner)
                    ghost_weight = pair_weights(left_sq, ghost_sq[...], dot_t(rows, ghosts[...]))
                    pulled = jnp.dot(
                        own_weight, own_aug[inside], preferred_element_type=jnp.float32
                    ) + jnp.dot(ghost_weight, ghost_aug[...], preferred_element_type=jnp.float32)
                    gain = gain_ref[source * capacity + slot]
                    forces = gain * (
                        pulled[:, :width] - pulled[:, width:] * rows.astype(jnp.float32)
                    )
                    held[source, slot] = forces.astype(jnp.bfloat16)

            out_copy(step, away).start()

    @pl.loop(0, steps + 1)
    def _(step):
        for half in range(halves):
            for offset in range(count_y):

                @pl.when(step == half * count_y + offset)
                def _():
                    forward(half, offset)

        @pl.when(step == 0)
        def _():
            ghost_aug[:, width:] = jnp.ones((ghost_aug.shape[0], width), jnp.bfloat16)
            own_aug[:, :, width:] = jnp.ones((group, block_rows, width), jnp.bfloat16)
            for copy in ghost_copies:
                copy.wait()
            for index in range(6):
                piece = ghosts[pl.ds(index * block_rows, block_rows), :]
                ghost_aug[pl.ds(index * block_rows, block_rows), pl.ds(0, width)] = piece
                _, row_sq = square_parts(dot_t(piece, piece))
                ghost_sq[:, pl.ds(index * block_rows, block_rows)] = row_sq

        for stage in range(3):

            @pl.when(step == 1 + (stage * steps) // 4)
            def _():
                hist_finish(stage)
                if stage < 2:
                    hist_start(stage + 1)

        @pl.when(step > 0)
        def _():
            compute(step - 1)

    for piece in pieces:
        z_copy(*piece).wait_send()

    @pl.loop(0, steps)
    def _(step):
        @pl.loop(0, plane)
        def _(away):
            @pl.when(away > 0)
            def _():
                forward_copy(step, away).wait_send()

            out_copy(step, away).wait()


def per_device(seg_rows, owner_map, ghost_pick, slab_cost):
    sizes = tuple(lax.axis_size(axis) for axis in AXES)
    count_x, count_y, count_z = sizes
    device_count = count_x * count_y * count_z
    blocks_here, block_rows, width = seg_rows.shape
    capacity = max(2, (2 * blocks_here + device_count - 1) // device_count)
    own_index = lax.axis_index(AXES)
    index_x = lax.axis_index("gx")
    index_y = lax.axis_index("gy")
    local_cost = slab_cost[0, 0, 0]
    bins_count = local_cost.shape[1]
    half_part = index_x // (count_x // 2)
    quarter = half_part * 2 + index_y // (count_y // 2)
    x_term = local_cost[0][None]
    y_term = jnp.where(
        lax.broadcasted_iota(jnp.int32, (2, bins_count), 0) == half_part, local_cost[1][None], 0
    )
    z_term = jnp.where(
        lax.broadcasted_iota(jnp.int32, (4, bins_count), 0) == quarter, local_cost[2][None], 0
    )
    terms = jnp.concatenate([x_term, y_term, z_term], axis=0).reshape(-1, LANES)
    exported = jnp.take(seg_rows, ghost_pick[0], axis=0)[0]

    all_owners = owner_map[:, 0].reshape(device_count, blocks_here)
    own_owners = lax.dynamic_index_in_dim(all_owners, own_index, 0, keepdims=False)
    block_order = lax.broadcasted_iota(jnp.int32, (blocks_here,), 0)
    earlier = block_order[:, None] < block_order[None, :]
    same_owner = own_owners[:, None] == own_owners[None, :]
    slot_rank = jnp.sum((same_owner & earlier).astype(jnp.int32), axis=0, dtype=jnp.int32)
    index_z = lax.axis_index("gz")
    plane = count_x * count_z
    plane_slots = plane * capacity

    def row_of(owner):
        return (owner // count_z) % count_y

    def spot_of(owner):
        return owner // (count_y * count_z) * count_z + owner % count_z

    own_offset = (row_of(own_owners) - index_y + count_y) % count_y
    own_spot = spot_of(own_owners)
    order = slot_rank * plane + own_spot
    ahead = (own_offset[:, None] == own_offset[None, :]) & (order[:, None] < order[None, :])
    compact = jnp.sum(ahead.astype(jnp.int32), axis=0, dtype=jnp.int32)
    place = jnp.where(own_offset == 0, own_spot * capacity + slot_rank, compact)
    place = own_offset * plane_slots + place
    place_ids = lax.broadcasted_iota(jnp.int32, (count_y * plane_slots,), 0)
    matches = place[None, :] == place_ids[:, None]
    pack_index = jnp.sum(jnp.where(matches, block_order[None, :], 0), axis=1, dtype=jnp.int32)

    line = lax.dynamic_index_in_dim(
        all_owners.reshape(count_x, count_y, count_z, blocks_here), index_x, 0, keepdims=False
    )
    line = lax.dynamic_index_in_dim(line, index_z, 1, keepdims=False)
    here = jnp.where(row_of(line) == index_y, spot_of(line), -1)
    spots = lax.broadcasted_iota(jnp.int32, (plane,), 0)
    ranks = lax.broadcasted_iota(jnp.int32, (capacity,), 0)
    named = jnp.sum(
        (here[:, None, :] == spots[None, :, None]).astype(jnp.int32), axis=2, dtype=jnp.int32
    )
    lower = jnp.sum(
        jnp.minimum(named[:, :, None], ranks[None, None, :]), axis=1, dtype=jnp.int32
    )
    beside = jnp.sum(
        (
            (named[:, None, :, None] > ranks[None, None, None, :])
            & (spots[None, None, :, None] < spots[None, :, None, None])
        ).astype(jnp.int32),
        axis=2,
        dtype=jnp.int32,
    )
    by_row = lower[:, None, :] + beside
    by_row = jnp.concatenate([by_row, by_row], axis=0)[::-1]
    forward_index = lax.dynamic_slice_in_dim(
        by_row, count_y - 1 - index_y, count_y, axis=0
    ).reshape(-1)

    all_rows = row_of(all_owners)
    source_rows = row_of(lax.broadcasted_iota(jnp.int32, (device_count, 1), 0))
    crowd = jnp.max(
        jnp.stack(
            [
                jnp.sum(((all_rows == row) & (source_rows != row)).astype(jnp.int32), axis=1)
                for row in range(count_y)
            ]
        )
    )
    arrivals = jnp.sum((all_owners == own_index).astype(jnp.int32), axis=1, dtype=jnp.int32)
    valid_slot = lax.broadcasted_iota(jnp.int32, (device_count, capacity), 1) < arrivals[:, None]
    gain = jnp.where(valid_slot, force_gain, 0.0).astype(jnp.float32).reshape(-1)

    halves = 2 if capacity % 2 == 0 else 1
    part = capacity // halves
    group = math.gcd(part, 2)
    first = plane * part
    rest = plane_slots - first
    limits = sorted({first + max(1, rest * share // 8) for share in SHARES}) if rest else [first]
    ghost_rows = 6 * block_rows
    hist_rows = terms.shape[0]
    hist_messages = sum(sizes) - 3
    steps = halves * count_y

    def relay(collective_id, limit):
        lengths = [first, limit - first][:halves]
        z_shapes = [
            pltpu.VMEM((length, block_rows, width), jnp.bfloat16)
            for length in lengths
            for _ in range(1, count_y)
        ]
        z_count = len(z_shapes)
        return pl.pallas_call(
            functools.partial(relay_kernel, sizes, capacity, halves, group, limit),
            out_shape=(
                jax.ShapeDtypeStruct((device_count, capacity, block_rows, width), jnp.bfloat16),
                jax.ShapeDtypeStruct((hist_rows, LANES), jnp.int32),
            ),
            in_specs=[pl.BlockSpec(memory_space=pltpu.SMEM)] * 3
            + [pl.BlockSpec(memory_space=pltpu.VMEM)] * 3,
            out_specs=(
                pl.BlockSpec(memory_space=pl.ANY),
                pl.BlockSpec(memory_space=pltpu.VMEM),
            ),
            scratch_shapes=[
                pltpu.VMEM((device_count, capacity, block_rows, width), jnp.bfloat16),
                pltpu.VMEM((steps, plane, part, block_rows, width), jnp.bfloat16),
                pltpu.VMEM((ghost_rows, width), jnp.bfloat16),
                pltpu.VMEM((ghost_rows, 2 * width), jnp.bfloat16),
                pltpu.VMEM((1, ghost_rows), jnp.float32),
                pltpu.VMEM((group, block_rows, 2 * width), jnp.bfloat16),
                pltpu.VMEM((2, hist_rows, LANES), jnp.int32),
                pltpu.VMEM((hist_messages, hist_rows, LANES), jnp.int32),
                pltpu.SemaphoreType.DMA((steps * plane,)),
                pltpu.SemaphoreType.DMA((steps * plane,)),
                pltpu.SemaphoreType.DMA((steps * plane,)),
                pltpu.SemaphoreType.DMA((z_count,)),
                pltpu.SemaphoreType.DMA((z_count,)),
                pltpu.SemaphoreType.DMA((6,)),
                pltpu.SemaphoreType.DMA((6,)),
                pltpu.SemaphoreType.DMA((hist_messages,)),
                pltpu.SemaphoreType.DMA((hist_messages,)),
            ]
            + z_shapes * 2,
            compiler_params=pltpu.CompilerParams(
                collective_id=collective_id,
                has_side_effects=True,
                vmem_limit_bytes=60 * 1024 * 1024,
            ),
            name=f"relay_forces_{limit}",
        )

    operands = (pack_index, forward_index, gain, seg_rows, exported, terms)
    if len(limits) > 1:
        choice = sum((crowd > limit).astype(jnp.int32) for limit in limits[:-1])
        forces, hist = lax.switch(
            choice, [relay(index, limit) for index, limit in enumerate(limits)], *operands
        )
    else:
        forces, hist = relay(0, limits[0])(*operands)
    extent = jnp.array([count_x, count_y, count_y, count_z, count_z, count_z, count_z], jnp.float32)
    cut_points = bisect_cuts(hist.reshape(-1, bins_count)) * extent
    return (forces[None], cut_points)


def solution(mesh):
    return jax.shard_map(
        per_device,
        mesh=mesh,
        in_specs=(
            P(AXES, None, None),
            P(),
            P(AXES, None),
            P("gx", "gy", "gz", None, None),
        ),
        out_specs=(P(AXES, None, None, None, None), P()),
        check_vma=False,
    )
```

```python
import functools
import math

import jax
import jax.numpy as jnp
from jax import lax
from jax.experimental import pallas as pl
from jax.experimental.pallas import tpu as pltpu
from jax.sharding import PartitionSpec as P

sharpness = 8.0
force_gain = 2.0
radius_eps = 0.001
AXES = ("gx", "gy", "gz")
MESH = pl.DeviceIdType.MESH
LANES = 128
SHARES = (3, 4, 8)


def bisect_cuts(histogram):
    running = jnp.cumsum(histogram, axis=1, dtype=jnp.int32)
    total_cost = running[:, -1]
    below = (2 * running < total_cost[:, None]).astype(jnp.int32)
    position = jnp.sum(below, axis=1, dtype=jnp.int32)
    before = jnp.sum(histogram * below, axis=1, dtype=jnp.int32)
    bins_index = lax.broadcasted_iota(jnp.int32, histogram.shape, 1)
    at_cut = jnp.sum(
        jnp.where(bins_index == position[:, None], histogram, 0), axis=1, dtype=jnp.int32
    )
    remain = (total_cost - 2 * before).astype(jnp.float32)
    return (
        position.astype(jnp.float32) + remain / (2 * at_cut).astype(jnp.float32)
    ) / histogram.shape[1]


def square_parts(inner):
    rows = lax.broadcasted_iota(jnp.int32, inner.shape, 0)
    columns = lax.broadcasted_iota(jnp.int32, inner.shape, 1)
    diagonal = jnp.where(rows == columns, inner, 0.0)
    return jnp.sum(diagonal, axis=1, keepdims=True), jnp.sum(diagonal, axis=0, keepdims=True)


def dot_t(left, right):
    return lax.dot_general(
        left, right, (((1,), (1,)), ((), ())), preferred_element_type=jnp.float32
    )


def pair_weights(left_sq, right_sq, inner):
    scale = sharpness * math.log2(math.e)
    ratio = (2.0 * inner + radius_eps) / (left_sq + (right_sq + radius_eps))
    return jnp.exp2(scale * ratio - scale).astype(jnp.bfloat16)


def relay_kernel(
    sizes, capacity, halves, group, limit,
    pack_ref, forward_ref, gain_ref, rows_ref, export_ref, cost_ref,
    forces_ref, hist_ref,
    held, stage_out, ghosts, ghost_aug, ghost_sq, own_aug, hist_cur, hist_in,
    send_sem, recv_sem, out_sem, zsend_sem, zrecv_sem,
    gsend_sem, grecv_sem, hsend_sem, hrecv_sem, *z_refs,
):
    count_x, count_y, count_z = sizes
    device_count = count_x * count_y * count_z
    plane = count_x * count_z
    part = capacity // halves
    plane_slots = plane * capacity
    first = plane * part
    block_rows, width = export_ref.shape
    coords = tuple(lax.axis_index(axis) for axis in AXES)
    me = (coords[0] * count_y + coords[1]) * count_z + coords[2]
    my_spot = coords[0] * count_z + coords[2]
    steps = halves * count_y
    bounds = [(0, first), (first, limit)][:halves]
    pieces = [(half, offset) for half in range(halves) for offset in range(1, count_y)]
    z_out = dict(zip(pieces, z_refs[: len(pieces)]))
    z_in = dict(zip(pieces, z_refs[len(pieces) :]))

    def coords_of(flat):
        return (flat // (count_y * count_z), (flat // count_z) % count_y, flat % count_z)

    def shifted(axis, offset):
        place = list(coords)
        place[axis] = (coords[axis] + offset + sizes[axis]) % sizes[axis]
        return tuple(place)

    barrier = pltpu.get_barrier_semaphore()

    @pl.loop(1, device_count)
    def _(k):
        pl.semaphore_signal(
            barrier, inc=1, device_id=coords_of((me + k) % device_count), device_id_type=MESH
        )

    def z_pack(half, offset):
        low, high = bounds[half]

        @pl.loop(0, high - low)
        def _(place):
            z_out[half, offset][place] = rows_ref[pack_ref[offset * plane_slots + low + place]]

    def z_copy(half, offset):
        index = pieces.index((half, offset))
        return pltpu.make_async_remote_copy(
            src_ref=z_out[half, offset],
            dst_ref=z_in[half, offset],
            send_sem=zsend_sem.at[index],
            recv_sem=zrecv_sem.at[index],
            device_id=shifted(1, offset),
            device_id_type=MESH,
        )

    z_pack(*pieces[0])
    pl.semaphore_wait(barrier, device_count - 1)

    ghost_copies = []
    for axis in range(3):
        for side, offset in ((0, 1), (1, -1)):
            index = 2 * axis + side
            copy = pltpu.make_async_remote_copy(
                src_ref=export_ref,
                dst_ref=ghosts.at[pl.ds(index * block_rows, block_rows)],
                send_sem=gsend_sem.at[index],
                recv_sem=grecv_sem.at[index],
                device_id=shifted(axis, offset),
                device_id_type=MESH,
            )
            copy.start()
            ghost_copies.append(copy)

    stage_axes = (1, 0, 2)
    bases = []
    total = 0
    for axis in stage_axes:
        bases.append(total)
        total += sizes[axis] - 1

    def hist_copies(stage):
        axis = stage_axes[stage]
        return [
            pltpu.make_async_remote_copy(
                src_ref=cost_ref if stage == 0 else hist_cur.at[stage - 1],
                dst_ref=hist_in.at[bases[stage] + offset - 1],
                send_sem=hsend_sem.at[bases[stage] + offset - 1],
                recv_sem=hrecv_sem.at[bases[stage] + offset - 1],
                device_id=shifted(axis, offset),
                device_id_type=MESH,
            )
            for offset in range(1, sizes[axis])
        ]

    def hist_start(stage):
        for copy in hist_copies(stage):
            copy.start()

    def hist_finish(stage):
        summed = cost_ref[...] if stage == 0 else hist_cur[stage - 1]
        for index, copy in enumerate(hist_copies(stage)):
            copy.wait()
            summed = summed + hist_in[bases[stage] + index]
        if stage == 2:
            hist_ref[...] = summed
        else:
            hist_cur[stage] = summed

    hist_start(0)
    for index, piece in enumerate(pieces):
        if index + 1 < len(pieces):
            z_pack(*pieces[index + 1])
        z_copy(*piece).start()

    def spot_shift(away):
        return (my_spot + away + plane) % plane

    def device_at(spot):
        return (spot // count_z, coords[1], spot % count_z)

    def source_at(spot, offset):
        row = (coords[1] - offset + count_y) % count_y
        return ((spot // count_z) * count_y + row) * count_z + spot % count_z

    def step_parts(step):
        later = (step // halves + count_y - 2) // (count_y - 1)
        turn = step - halves + halves * (count_y - 1)
        half = (1 - later) * step + later * (turn // (count_y - 1) - halves)
        return half, later * (turn % (count_y - 1) + 1)

    def forward_copy(step, away):
        half, offset = step_parts(step)
        spot = spot_shift(away)
        return pltpu.make_async_remote_copy(
            src_ref=stage_out.at[step, away],
            dst_ref=held.at[source_at(my_spot, offset), pl.ds(half * part, part)],
            send_sem=send_sem.at[step * plane + away],
            recv_sem=recv_sem.at[step * plane + away],
            device_id=device_at(spot),
            device_id_type=MESH,
        )

    def arrival(step, away):
        half, offset = step_parts(step)
        spot = spot_shift(-away)
        return pltpu.make_async_remote_copy(
            src_ref=stage_out.at[step, away],
            dst_ref=held.at[source_at(spot, offset), pl.ds(half * part, part)],
            send_sem=send_sem.at[step * plane + away],
            recv_sem=recv_sem.at[step * plane + away],
            device_id=device_at(spot),
            device_id_type=MESH,
        )

    def slot_value(half, offset, spot, inside):
        index = spot * capacity + half * part + inside
        if offset == 0:
            return rows_ref[pack_ref[index]]
        place = forward_ref[offset * plane_slots + index]
        if half == 0:
            return z_in[0, offset][place]
        early = z_in[0, offset][jnp.minimum(place, first - 1)]
        late = z_in[1, offset][jnp.clip(place - first, 0, limit - first - 1)]
        is_early = jnp.full(early.shape, place, jnp.int32) < first
        return jnp.where(is_early, early, late)

    def step_of(half, offset):
        return half if offset == 0 else halves + half * (count_y - 1) + offset - 1

    def turn_of(half, offset):
        step = step_of(half, offset)
        if step < halves:
            return 0
        return step if step <= halves + count_y - 2 else step - 1

    def forward(half, offset):
        step = step_of(half, offset)
        if offset > 0:
            z_copy(half, offset).wait_recv()

        @pl.loop(1, plane)
        def _(away):
            for inside in range(part):
                stage_out[step, away, inside] = slot_value(half, offset, spot_shift(away), inside)

            @pl.when(away > 1)
            def _():
                forward_copy(step, away - 1).start()

        own = source_at(my_spot, offset)
        for inside in range(part):
            held[own, half * part + inside] = slot_value(half, offset, my_spot, inside)
        forward_copy(step, plane - 1).start()

    def out_copy(step, away):
        half, offset = step_parts(step)
        source = source_at(spot_shift(-away), offset)
        return pltpu.make_async_copy(
            held.at[source, pl.ds(half * part, part)],
            forces_ref.at[source, pl.ds(half * part, part)],
            out_sem.at[step * plane + away],
        )

    def compute(step):
        half, offset = step_parts(step)

        @pl.loop(0, plane)
        def _(away):
            source = source_at(spot_shift(-away), offset)

            @pl.when(away > 0)
            def _():
                arrival(step, away).wait_recv()

            @pl.loop(0, part // group)
            def _(pair):
                for inside in range(group):
                    slot = half * part + pair * group + inside
                    rows = held[source, slot]
                    own_aug[inside, :, pl.ds(0, width)] = rows
                    own_inner = dot_t(rows, rows)
                    left_sq, right_sq = square_parts(own_inner)
                    own_weight = pair_weights(left_sq, right_sq, own_inner)
                    ghost_weight = pair_weights(left_sq, ghost_sq[...], dot_t(rows, ghosts[...]))
                    pulled = jnp.dot(
                        own_weight, own_aug[inside], preferred_element_type=jnp.float32
                    ) + jnp.dot(ghost_weight, ghost_aug[...], preferred_element_type=jnp.float32)
                    gain = gain_ref[source * capacity + slot]
                    forces = gain * (
                        pulled[:, :width] - pulled[:, width:] * rows.astype(jnp.float32)
                    )
                    held[source, slot] = forces.astype(jnp.bfloat16)

            out_copy(step, away).start()

    @pl.loop(0, steps)
    def _(step):
        for half, offset in [(half, 0) for half in range(halves)] + pieces:

            @pl.when(step == turn_of(half, offset))
            def _():
                forward(half, offset)

        @pl.when(step == 0)
        def _():
            ghost_aug[:, width:] = jnp.ones((ghost_aug.shape[0], width), jnp.bfloat16)
            own_aug[:, :, width:] = jnp.ones((group, block_rows, width), jnp.bfloat16)
            for copy in ghost_copies:
                copy.wait()
            for index in range(6):
                piece = ghosts[pl.ds(index * block_rows, block_rows), :]
                ghost_aug[pl.ds(index * block_rows, block_rows), pl.ds(0, width)] = piece
                _, row_sq = square_parts(dot_t(piece, piece))
                ghost_sq[:, pl.ds(index * block_rows, block_rows)] = row_sq

        for stage in range(3):

            @pl.when(step == 1 + (stage * steps) // 4)
            def _():
                hist_finish(stage)
                if stage < 2:
                    hist_start(stage + 1)

        compute(step)

    for piece in pieces:
        z_copy(*piece).wait_send()

    @pl.loop(0, steps)
    def _(step):
        @pl.loop(0, plane)
        def _(away):
            @pl.when(away > 0)
            def _():
                forward_copy(step, away).wait_send()

            out_copy(step, away).wait()


def per_device(seg_rows, owner_map, ghost_pick, slab_cost):
    sizes = tuple(lax.axis_size(axis) for axis in AXES)
    count_x, count_y, count_z = sizes
    device_count = count_x * count_y * count_z
    blocks_here, block_rows, width = seg_rows.shape
    capacity = max(2, (2 * blocks_here + device_count - 1) // device_count)
    own_index = lax.axis_index(AXES)
    index_x = lax.axis_index("gx")
    index_y = lax.axis_index("gy")
    local_cost = slab_cost[0, 0, 0]
    bins_count = local_cost.shape[1]
    half_part = index_x // (count_x // 2)
    quarter = half_part * 2 + index_y // (count_y // 2)
    x_term = local_cost[0][None]
    y_term = jnp.where(
        lax.broadcasted_iota(jnp.int32, (2, bins_count), 0) == half_part, local_cost[1][None], 0
    )
    z_term = jnp.where(
        lax.broadcasted_iota(jnp.int32, (4, bins_count), 0) == quarter, local_cost[2][None], 0
    )
    terms = jnp.concatenate([x_term, y_term, z_term], axis=0).reshape(-1, LANES)
    exported = jnp.take(seg_rows, ghost_pick[0], axis=0)[0]

    all_owners = owner_map[:, 0].reshape(device_count, blocks_here)
    own_owners = lax.dynamic_index_in_dim(all_owners, own_index, 0, keepdims=False)
    block_order = lax.broadcasted_iota(jnp.int32, (blocks_here,), 0)
    earlier = block_order[:, None] < block_order[None, :]
    same_owner = own_owners[:, None] == own_owners[None, :]
    slot_rank = jnp.sum((same_owner & earlier).astype(jnp.int32), axis=0, dtype=jnp.int32)
    index_z = lax.axis_index("gz")
    plane = count_x * count_z
    plane_slots = plane * capacity

    def row_of(owner):
        return (owner // count_z) % count_y

    def spot_of(owner):
        return owner // (count_y * count_z) * count_z + owner % count_z

    own_offset = (row_of(own_owners) - index_y + count_y) % count_y
    own_spot = spot_of(own_owners)
    order = slot_rank * plane + own_spot
    ahead = (own_offset[:, None] == own_offset[None, :]) & (order[:, None] < order[None, :])
    compact = jnp.sum(ahead.astype(jnp.int32), axis=0, dtype=jnp.int32)
    place = jnp.where(own_offset == 0, own_spot * capacity + slot_rank, compact)
    place = own_offset * plane_slots + place
    place_ids = lax.broadcasted_iota(jnp.int32, (count_y * plane_slots,), 0)
    matches = place[None, :] == place_ids[:, None]
    pack_index = jnp.sum(jnp.where(matches, block_order[None, :], 0), axis=1, dtype=jnp.int32)

    line = lax.dynamic_index_in_dim(
        all_owners.reshape(count_x, count_y, count_z, blocks_here), index_x, 0, keepdims=False
    )
    line = lax.dynamic_index_in_dim(line, index_z, 1, keepdims=False)
    here = jnp.where(row_of(line) == index_y, spot_of(line), -1)
    spots = lax.broadcasted_iota(jnp.int32, (plane,), 0)
    ranks = lax.broadcasted_iota(jnp.int32, (capacity,), 0)
    named = jnp.sum(
        (here[:, None, :] == spots[None, :, None]).astype(jnp.int32), axis=2, dtype=jnp.int32
    )
    lower = jnp.sum(
        jnp.minimum(named[:, :, None], ranks[None, None, :]), axis=1, dtype=jnp.int32
    )
    beside = jnp.sum(
        (
            (named[:, None, :, None] > ranks[None, None, None, :])
            & (spots[None, None, :, None] < spots[None, :, None, None])
        ).astype(jnp.int32),
        axis=2,
        dtype=jnp.int32,
    )
    by_row = lower[:, None, :] + beside
    by_row = jnp.concatenate([by_row, by_row], axis=0)[::-1]
    forward_index = lax.dynamic_slice_in_dim(
        by_row, count_y - 1 - index_y, count_y, axis=0
    ).reshape(-1)

    all_rows = row_of(all_owners)
    source_rows = row_of(lax.broadcasted_iota(jnp.int32, (device_count, 1), 0))
    crowd = jnp.max(
        jnp.stack(
            [
                jnp.sum(((all_rows == row) & (source_rows != row)).astype(jnp.int32), axis=1)
                for row in range(count_y)
            ]
        )
    )
    arrivals = jnp.sum((all_owners == own_index).astype(jnp.int32), axis=1, dtype=jnp.int32)
    valid_slot = lax.broadcasted_iota(jnp.int32, (device_count, capacity), 1) < arrivals[:, None]
    gain = jnp.where(valid_slot, force_gain, 0.0).astype(jnp.float32).reshape(-1)

    halves = 2 if capacity % 2 == 0 else 1
    part = capacity // halves
    group = math.gcd(part, 2)
    first = plane * part
    rest = plane_slots - first
    limits = sorted({first + max(1, rest * share // 8) for share in SHARES}) if rest else [first]
    ghost_rows = 6 * block_rows
    hist_rows = terms.shape[0]
    hist_messages = sum(sizes) - 3
    steps = halves * count_y

    def relay(collective_id, limit):
        lengths = [first, limit - first][:halves]
        z_shapes = [
            pltpu.VMEM((length, block_rows, width), jnp.bfloat16)
            for length in lengths
            for _ in range(1, count_y)
        ]
        z_count = len(z_shapes)
        return pl.pallas_call(
            functools.partial(relay_kernel, sizes, capacity, halves, group, limit),
            out_shape=(
                jax.ShapeDtypeStruct((device_count, capacity, block_rows, width), jnp.bfloat16),
                jax.ShapeDtypeStruct((hist_rows, LANES), jnp.int32),
            ),
            in_specs=[pl.BlockSpec(memory_space=pltpu.SMEM)] * 3
            + [pl.BlockSpec(memory_space=pltpu.VMEM)] * 3,
            out_specs=(
                pl.BlockSpec(memory_space=pl.ANY),
                pl.BlockSpec(memory_space=pltpu.VMEM),
            ),
            scratch_shapes=[
                pltpu.VMEM((device_count, capacity, block_rows, width), jnp.bfloat16),
                pltpu.VMEM((steps, plane, part, block_rows, width), jnp.bfloat16),
                pltpu.VMEM((ghost_rows, width), jnp.bfloat16),
                pltpu.VMEM((ghost_rows, 2 * width), jnp.bfloat16),
                pltpu.VMEM((1, ghost_rows), jnp.float32),
                pltpu.VMEM((group, block_rows, 2 * width), jnp.bfloat16),
                pltpu.VMEM((2, hist_rows, LANES), jnp.int32),
                pltpu.VMEM((hist_messages, hist_rows, LANES), jnp.int32),
                pltpu.SemaphoreType.DMA((steps * plane,)),
                pltpu.SemaphoreType.DMA((steps * plane,)),
                pltpu.SemaphoreType.DMA((steps * plane,)),
                pltpu.SemaphoreType.DMA((z_count,)),
                pltpu.SemaphoreType.DMA((z_count,)),
                pltpu.SemaphoreType.DMA((6,)),
                pltpu.SemaphoreType.DMA((6,)),
                pltpu.SemaphoreType.DMA((hist_messages,)),
                pltpu.SemaphoreType.DMA((hist_messages,)),
            ]
            + z_shapes * 2,
            compiler_params=pltpu.CompilerParams(
                collective_id=collective_id,
                has_side_effects=True,
                vmem_limit_bytes=60 * 1024 * 1024,
            ),
            name=f"relay_forces_{limit}",
        )

    operands = (pack_index, forward_index, gain, seg_rows, exported, terms)
    if len(limits) > 1:
        choice = sum((crowd > limit).astype(jnp.int32) for limit in limits[:-1])
        forces, hist = lax.switch(
            choice, [relay(index, limit) for index, limit in enumerate(limits)], *operands
        )
    else:
        forces, hist = relay(0, limits[0])(*operands)
    extent = jnp.array([count_x, count_y, count_y, count_z, count_z, count_z, count_z], jnp.float32)
    cut_points = bisect_cuts(hist.reshape(-1, bins_count)) * extent
    return (forces[None], cut_points)


def solution(mesh):
    return jax.shard_map(
        per_device,
        mesh=mesh,
        in_specs=(
            P(AXES, None, None),
            P(),
            P(AXES, None),
            P("gx", "gy", "gz", None, None),
        ),
        out_specs=(P(AXES, None, None, None, None), P()),
        check_vma=False,
    )
```
